512 devices in a mesh: head: 8 (over x, core), tok: 64 (over z, y).
Axes of the slice: x: 4, y: 8, z: 8, core: 2. Of those that a mesh axis runs over, the one named last changes fastest.
Arguments:
- queries: bfloat16 [49152, 1024], P('tok', 'head'), may hold values from -512 to 512
- keys: bfloat16 [49152, 1024], P('tok', 'head'), may hold values from -8 to 8
- values: bfloat16 [49152, 1024], P('tok', 'head'), may hold values from -6 to 6
- out_grad: bfloat16 [49152, 1024], P('tok', 'head'), may hold values from -6 to 6
- w_query: bfloat16 [1024, 1024], P(None, 'head'), may hold values from -0.1875 to 0.1875
- w_key: bfloat16 [1024, 1024], P(None, 'head'), may hold values from -0.1875 to 0.1875
- w_value: bfloat16 [1024, 1024], P(None, 'head'), may hold values from -0.1875 to 0.1875
- w_out: bfloat16 [1024, 1024], P('head'), may hold values from -0.1875 to 0.1875
- page_cluster: int32 [1536], replicated, may hold values from 0 to 63, as said below
Outputs:
- input_grad: bfloat16 [49152, 1024], P('tok', 'head')
The draws below stay inside these ranges and needn't reach their ends.
Inputs may be any that keep to these rules, and one draw needn't show every extreme that they name: `page_cluster`: the 24 pages k * 24 to k * 24 + 23, for each k, name distinct clusters. No cluster is named by more than 32 pages, and some cluster by exactly 32.
All inputs are finite; a program needn't handle non-finite values.
Results may differ from the reference program's by a relative error of at most 0.014.
Values may be sent and summed in bfloat16 or wider, within the bound.
No kernel may reach another device: no remote copies, remote signals or barrier semaphores. Data moves between devices by JAX's collectives and lax.ppermute only.
A program may use at most 64 MiB of HBM per device.

```python
import jax
import jax.numpy as jnp
from jax import lax

D = 1024
HEADS = 8
HEAD_DIM = 128
PAGE = 32
PAGES_DEV = 24
CLUSTER_PAGES = 32
TOKENS = 49152
CLUSTERS = 64
CLUSTER = 1024
N_HEAD = 8


def draw_page_cluster(key, part):
    clusters = CLUSTERS
    per_device = PAGES_DEV
    donors = CLUSTER_PAGES - per_device
    sorted_label = jnp.arange(clusters, dtype=jnp.int32)
    counts = jnp.where(sorted_label == 0, CLUSTER_PAGES, jnp.where(sorted_label <= donors, per_device - 1, per_device))
    offset = sorted_label - (donors + 1)
    pair_index = jnp.maximum(offset, 0) // 2
    amount_cap = min(per_device - 1, CLUSTER_PAGES - per_device)
    amounts = jax.random.randint(jax.random.fold_in(key, 3), (clusters,), 0, amount_cap + 1)
    amount = amounts[pair_index]
    direction = jnp.where(offset < 0, 0, jnp.where(offset % 2 == 0, jnp.where(sorted_label + 1 < clusters, 1, 0), -1))
    counts = counts + direction * amount
    run_ends = jnp.cumsum(counts)
    entry_order = jnp.arange(clusters * per_device, dtype=jnp.int32)
    entry_label = jnp.sum((run_ends[None, :] <= entry_order[:, None]).astype(jnp.int32), axis=1)
    shuffle = jax.random.permutation(jax.random.fold_in(key, 5), clusters)
    chosen = shuffle[entry_label].reshape(per_device, clusters)
    rotation = jax.random.randint(jax.random.fold_in(key, 4), (), 0, clusters)
    chosen = jnp.roll(chosen, rotation, axis=1)
    return chosen.T.reshape(clusters * per_device).astype(jnp.int32)


def drawn_normal(key, shape):
    return jnp.clip(jax.random.normal(key, shape, jnp.float32), -6.0, 6.0)


def draw_keys(key, part):
    drawn = drawn_normal(jax.random.fold_in(key, 7), (TOKENS, HEADS * HEAD_DIM))
    return drawn.astype(jnp.bfloat16)


def draw_queries(key, part):
    drawn = drawn_normal(jax.random.fold_in(key, 9), (TOKENS, HEADS * HEAD_DIM))
    return drawn.astype(jnp.bfloat16)


def level_of(key, dims, shards, smallest, top_value):
    def one(dim, parts):
        heights = jax.random.uniform(jax.random.fold_in(jax.random.fold_in(key, 6), dim), (parts,), jnp.float32, smallest / len(shards), top_value / len(shards))
        return jnp.repeat(jnp.exp(heights), dims[dim] // parts).reshape((-1,) + (1,) * (len(dims) - dim - 1))

    gain = one(*shards[0])
    for cut in shards[1:]:
        gain = gain * one(*cut)
    return gain


def bell_draw(rng, shape, scale, reach, shards=(), held_as=jnp.bfloat16):
    values = scale * jax.random.normal(rng, shape, jnp.float32)
    if shards:
        values = values * level_of(rng, shape, shards, -0.22, 0.18)
    return jnp.clip(values, -reach, reach).astype(held_as)


def setup_inputs(seed: int = 0) -> dict:
    seeds = jax.random.split(jax.random.key(seed), 10)
    return {
        "queries": draw_queries(jax.random.fold_in(seeds[9], 71), 0),
        "keys": draw_keys(jax.random.fold_in(seeds[9], 71), 0),
        "values": bell_draw(seeds[2], (TOKENS, HEADS * HEAD_DIM), 1.0, 6.0, ((0, 64), (1, 8))),
        "out_grad": bell_draw(seeds[3], (TOKENS, D), 1.0, 6.0, ((0, 64), (1, 8))),
        "w_query": bell_draw(seeds[4], (D, HEADS * HEAD_DIM), D ** -0.5, 0.1875, ((1, 8),)),
        "w_key": bell_draw(seeds[5], (D, HEADS * HEAD_DIM), D ** -0.5, 0.1875, ((1, 8),)),
        "w_value": bell_draw(seeds[6], (D, HEADS * HEAD_DIM), D ** -0.5, 0.1875, ((1, 8),)),
        "w_out": bell_draw(seeds[7], (HEADS * HEAD_DIM, D), (HEADS * HEAD_DIM) ** -0.5, 0.1875, ((0, 8),)),
        "page_cluster": draw_page_cluster(jax.random.fold_in(seeds[9], 71), 0),
    }


def page_ranks(page_cluster):
    page_order = jnp.arange(page_cluster.shape[0], dtype=jnp.int32)
    same_cluster = page_cluster[:, None] == page_cluster[None, :]
    earlier = page_order[None, :] < page_order[:, None]
    return jnp.sum((same_cluster & earlier).astype(jnp.int32), axis=1)


def slot_tables(page_cluster, page_rank):
    page_order = jnp.arange(page_cluster.shape[0], dtype=jnp.int32)
    cluster_order = jnp.arange(CLUSTERS, dtype=jnp.int32)
    slot_order = jnp.arange(CLUSTER_PAGES, dtype=jnp.int32)
    slot_hit = (page_cluster[None, None, :] == cluster_order[:, None, None]) & (page_rank[None, None, :] == slot_order[None, :, None])
    filled = jnp.any(slot_hit, axis=2)
    slot_page = jnp.sum(slot_hit.astype(jnp.int32) * page_order[None, None, :], axis=2).astype(jnp.int32)
    return slot_page, filled


def head_backward(query_head, key_head, value_head, grad_head, page_cluster, slot_page, filled):
    page_total = TOKENS // PAGE
    query_pages = query_head.reshape(page_total, PAGE, HEAD_DIM)
    key_pages = key_head.reshape(page_total, PAGE, HEAD_DIM)
    value_pages = value_head.reshape(page_total, PAGE, HEAD_DIM)
    grad_pages = grad_head.reshape(page_total, PAGE, HEAD_DIM)
    inner_index = jnp.arange(PAGE, dtype=jnp.int32)
    score_scale = HEAD_DIM ** -0.5

    def page_step(running, page_number):
        dkey_sum, dvalue_sum = running
        cluster_id = page_cluster[page_number]
        key_list = slot_page[cluster_id]
        key_valid = filled[cluster_id]
        query_rows = query_pages[page_number].astype(jnp.float32)
        grad_rows = grad_pages[page_number].astype(jnp.float32)
        key_rows = key_pages[key_list].reshape(CLUSTER, HEAD_DIM).astype(jnp.float32)
        value_rows = value_pages[key_list].reshape(CLUSTER, HEAD_DIM).astype(jnp.float32)
        query_pos = page_number * PAGE + inner_index
        key_pos = (key_list[:, None] * PAGE + inner_index[None, :]).reshape(CLUSTER)
        key_live = jnp.broadcast_to(key_valid[:, None], (CLUSTER_PAGES, PAGE)).reshape(CLUSTER)
        allowed = key_live[None, :] & (key_pos[None, :] <= query_pos[:, None])
        score = jnp.dot(query_rows, key_rows.T, preferred_element_type=jnp.float32) * score_scale
        score = jnp.where(allowed, score, -1e30)
        row_max = jnp.max(score, axis=1, keepdims=True)
        raised = jnp.where(allowed, jnp.exp(score - row_max), 0.0)
        weights = raised / jnp.sum(raised, axis=1, keepdims=True)
        weights_half = lax.optimization_barrier(weights.astype(jnp.bfloat16)).astype(jnp.float32)
        grad_weights = jnp.dot(grad_rows, value_rows.T, preferred_element_type=jnp.float32)
        row_delta = jnp.sum(weights * grad_weights, axis=1, keepdims=True)
        grad_score = lax.optimization_barrier((weights * (grad_weights - row_delta)).astype(jnp.bfloat16)).astype(jnp.float32)
        dquery = (jnp.dot(grad_score, key_rows, preferred_element_type=jnp.float32) * score_scale).astype(jnp.bfloat16)
        dkey_part = jnp.dot(grad_score.T, query_rows, preferred_element_type=jnp.float32) * score_scale
        dvalue_part = jnp.dot(weights_half.T, grad_rows, preferred_element_type=jnp.float32)
        dkey_sum = dkey_sum.at[key_list].add(dkey_part.reshape(CLUSTER_PAGES, PAGE, HEAD_DIM))
        dvalue_sum = dvalue_sum.at[key_list].add(dvalue_part.reshape(CLUSTER_PAGES, PAGE, HEAD_DIM))
        return (dkey_sum, dvalue_sum), dquery

    start_sums = (jnp.zeros((page_total, PAGE, HEAD_DIM), jnp.float32), jnp.zeros((page_total, PAGE, HEAD_DIM), jnp.float32))
    sums, dquery = lax.scan(page_step, start_sums, jnp.arange(page_total, dtype=jnp.int32))
    dkey = sums[0].reshape(TOKENS, HEAD_DIM).astype(jnp.bfloat16)
    dvalue = sums[1].reshape(TOKENS, HEAD_DIM).astype(jnp.bfloat16)
    return dquery.reshape(TOKENS, HEAD_DIM), dkey, dvalue


def reference(queries, keys, values, out_grad, w_query, w_key, w_value, w_out, page_cluster):
    grad_heads = jnp.dot(out_grad, w_out.T, preferred_element_type=jnp.float32).astype(jnp.bfloat16)
    page_rank = page_ranks(page_cluster)
    slot_page, filled = slot_tables(page_cluster, page_rank)

    def split_heads(matrix):
        return matrix.reshape(TOKENS, HEADS, HEAD_DIM).transpose(1, 0, 2)

    def join_heads(matrix):
        return matrix.transpose(1, 0, 2).reshape(TOKENS, HEADS * HEAD_DIM)

    def one_head(items):
        return head_backward(items[0], items[1], items[2], items[3], page_cluster, slot_page, filled)

    stacked = (split_heads(queries), split_heads(keys), split_heads(values), split_heads(grad_heads))
    dquery, dkey, dvalue = lax.map(one_head, stacked)
    dquery = join_heads(dquery)
    dkey = join_heads(dkey)
    dvalue = join_heads(dvalue)
    group_cols = (HEADS // N_HEAD) * HEAD_DIM
    total = jnp.zeros((TOKENS, D), jnp.float32)
    for group_index in range(N_HEAD):
        low = group_index * group_cols
        high = low + group_cols
        partial_value = jnp.dot(dquery[:, low:high], w_query[:, low:high].T, preferred_element_type=jnp.float32)
        partial_value = partial_value + jnp.dot(dkey[:, low:high], w_key[:, low:high].T, preferred_element_type=jnp.float32)
        partial_value = partial_value + jnp.dot(dvalue[:, low:high], w_value[:, low:high].T, preferred_element_type=jnp.float32)
        partial_value = lax.optimization_barrier(partial_value.astype(jnp.bfloat16))
        total = total + partial_value.astype(jnp.float32)
    return total.astype(jnp.bfloat16)
```

```python
import math

import jax
import jax.numpy as jnp
from jax import lax
from jax.experimental import pallas as pl
from jax.experimental.pallas import tpu as pltpu
from jax.sharding import PartitionSpec as P

HEAD_DIM = 128
PAGE = 32
SLOTS = 32
BLOCK = 256
NEG = -1e30
VMEM = pl.BlockSpec(memory_space=pltpu.VMEM)
SMEM = pl.BlockSpec(memory_space=pltpu.SMEM)


def mm(a, b, dims):
    return lax.dot_general(a, b, (dims, ((), ())), preferred_element_type=jnp.float32)


def rows(page):
    return pl.ds(pl.multiple_of(page * PAGE, PAGE), PAGE)


def pack_kernel(dest, core, query, key, value, even, odd, w_out, sent, grad):
    count = even.shape[0]
    total = None
    for x in range(count):
        for got, side in ((even, core[0]), (odd, 1 - core[0])):
            part = mm(got[x], w_out[2 * x + side], ((1,), (1,)))
            total = part if total is None else total + part
    grad[...] = total.astype(grad.dtype)
    for page in range(dest.shape[0]):
        peer = dest[page]
        for part, array in enumerate((query, key, value, grad)):
            sent[peer, part * PAGE : (part + 1) * PAGE] = array[page * PAGE : (page + 1) * PAGE]


def attention_kernel(source, arrived, grads, query, key, value, grad, dkey, dvalue):
    scale = HEAD_DIM ** (-0.5)
    arrays = (query, key, value, grad)

    def assemble(slot, carry):
        peer = source[slot]

        @pl.when(peer >= 0)
        def _():
            for part, array in enumerate(arrays):
                array[rows(slot)] = arrived[peer, part * PAGE : (part + 1) * PAGE]

        @pl.when(peer < 0)
        def _():
            for array in arrays:
                array[rows(slot)] = jnp.zeros((PAGE, HEAD_DIM), array.dtype)

        return carry

    lax.fori_loop(0, source.shape[0], assemble, 0)
    total = query.shape[0]
    block = min(BLOCK, total)
    row_order = lax.broadcasted_iota(jnp.int32, (block, block), 0)
    causal = lax.broadcasted_iota(jnp.int32, (block, block), 1) <= row_order
    for first in range(0, total, block):
        last = first + block
        here = slice(first, last)
        spans = ([slice(0, first)] if first else []) + [here]
        part_query, part_grad = query[here], grad[here]
        score = [mm(part_query, key[span], ((1,), (1,))) for span in spans]
        score[-1] = jnp.where(causal, score[-1], NEG)
        row_max = score[-1].max(axis=1, keepdims=True)
        if first:
            row_max = jnp.maximum(row_max, score[0].max(axis=1, keepdims=True))
        raised = [jnp.exp2((s - row_max) * (scale * math.log2(math.e))) for s in score]
        row_sum = sum(r.sum(axis=1, keepdims=True) for r in raised)
        inverse = 1.0 / row_sum
        weights = [r * inverse for r in raised]
        grad_weights = [mm(part_grad, value[span], ((1,), (1,))) for span in spans]
        row_delta = sum((w * g).sum(axis=1, keepdims=True) for w, g in zip(weights, grad_weights))
        grad_score = [
            (w * (g - row_delta)).astype(jnp.bfloat16) for w, g in zip(weights, grad_weights)
        ]
        dquery = sum(mm(d, key[span], ((1,), (0,))) for d, span in zip(grad_score, spans))
        grads[here, 0:HEAD_DIM] = (dquery * scale).astype(grads.dtype)
        for w, d, span in zip(weights, grad_score, spans):
            more_key = mm(d, part_query, ((0,), (0,)))
            more_value = mm(w.astype(jnp.bfloat16), part_grad, ((0,), (0,)))
            if span is here:
                dkey[span] = more_key
                dvalue[span] = more_value
            else:
                dkey[span] += more_key
                dvalue[span] += more_value
    grads[:, HEAD_DIM : 2 * HEAD_DIM] = (dkey[...] * scale).astype(grads.dtype)
    grads[:, 2 * HEAD_DIM : 3 * HEAD_DIM] = dvalue[...].astype(grads.dtype)


def project_kernel(mine, theirs, w_mine, w_theirs, out):
    total = mm(mine[...], w_mine[...], ((1,), (1,))) + mm(theirs[...], w_theirs[...], ((1,), (1,)))
    for x in range(out.shape[0]):
        out[x] = total[:, x * HEAD_DIM : (x + 1) * HEAD_DIM].astype(out.dtype)


def sum_kernel(source, parts, sent):
    def one(slot, carry):
        peer = source[slot]

        @pl.when(peer >= 0)
        def _():
            total = parts[0, rows(slot)].astype(jnp.float32)
            for x in range(1, parts.shape[0]):
                total = total + parts[x, rows(slot)].astype(jnp.float32)
            sent[peer] = total.astype(sent.dtype)

        return carry

    lax.fori_loop(0, source.shape[0], one, 0)


def unpack_kernel(dest, returned, out):
    for page in range(dest.shape[0]):
        out[page * PAGE : (page + 1) * PAGE] = returned[dest[page]]


def per_device(queries, keys, values, out_grad, w_query, w_key, w_value, w_out, page_cluster):
    tok_rows = queries.shape[0]
    pages_here = tok_rows // PAGE
    peers = lax.axis_size("tok")
    heads = lax.axis_size("head")
    chips = heads // 2
    myself = lax.axis_index("tok")
    core = lax.axis_index("head") % 2
    across = [[2 * x + side for x in range(chips)] for side in range(2)]
    swap = [(h, h ^ 1) for h in range(heads)]
    slot_rows = SLOTS * PAGE
    half = queries.dtype

    table = page_cluster.reshape(peers, pages_here)
    dest = lax.dynamic_index_in_dim(table, myself, 0, keepdims=False)
    has = jnp.any(table == myself, axis=1).astype(jnp.int32)
    peer_order = jnp.arange(peers, dtype=jnp.int32)
    rank = jnp.sum(jnp.where(peer_order[:, None] < peer_order[None, :], has[:, None], 0), axis=0)
    slot_order = jnp.arange(SLOTS, dtype=jnp.int32)
    hit = (rank[None, :] == slot_order[:, None]) & (has[None, :] == 1)
    source = jnp.sum(jnp.where(hit, peer_order[None, :] + 1, 0), axis=1) - 1

    w_blocks = w_out.reshape(HEAD_DIM, heads, HEAD_DIM).transpose(1, 0, 2)

    same_core = lax.all_to_all(
        jnp.broadcast_to(out_grad[None], (chips, *out_grad.shape)),
        "head", 0, 0, axis_index_groups=across, tiled=True,
    )
    other_core = lax.ppermute(same_core, "head", swap)
    sent = pl.pallas_call(
        pack_kernel,
        out_shape=jax.ShapeDtypeStruct((peers, 4 * PAGE, HEAD_DIM), half),
        in_specs=[SMEM, SMEM] + [VMEM] * 6,
        out_specs=VMEM,
        scratch_shapes=[pltpu.VMEM((tok_rows, HEAD_DIM), half)],
        name="pack",
    )(dest, core[None], queries, keys, values, same_core, other_core, w_blocks)
    sent, w_query, w_key, w_value = lax.optimization_barrier((sent, w_query, w_key, w_value))
    arrived = lax.all_to_all(sent, "tok", 0, 0, tiled=True)
    weights = jnp.concatenate([w_query, w_key, w_value], axis=1)
    weights = weights.reshape(chips, 2, HEAD_DIM, 3 * HEAD_DIM)
    w_mine = lax.dynamic_index_in_dim(weights, core, 1, keepdims=False)
    w_away = lax.dynamic_index_in_dim(weights, 1 - core, 1, keepdims=False)
    w_theirs = lax.ppermute(w_away, "head", swap)
    w_mine = w_mine.reshape(chips * HEAD_DIM, 3 * HEAD_DIM)
    w_theirs = w_theirs.reshape(chips * HEAD_DIM, 3 * HEAD_DIM)
    arrived, w_mine, w_theirs = lax.optimization_barrier((arrived, w_mine, w_theirs))
    grads = pl.pallas_call(
        attention_kernel,
        out_shape=jax.ShapeDtypeStruct((slot_rows, 3 * HEAD_DIM), half),
        in_specs=[SMEM, VMEM],
        out_specs=VMEM,
        scratch_shapes=[pltpu.VMEM((slot_rows, HEAD_DIM), half)] * 4
        + [pltpu.VMEM((slot_rows, HEAD_DIM), jnp.float32)] * 2,
        name="attention",
    )(source, arrived)
    their_grads = lax.ppermute(grads, "head", swap)
    step = min(BLOCK, slot_rows)
    row_block = pl.BlockSpec((step, 3 * HEAD_DIM), lambda i: (i, 0))
    w_block = pl.BlockSpec(w_mine.shape, lambda i: (0, 0))
    partial = pl.pallas_call(
        project_kernel,
        out_shape=jax.ShapeDtypeStruct((chips, slot_rows, HEAD_DIM), half),
        grid=(slot_rows // step,),
        in_specs=[row_block, row_block, w_block, w_block],
        out_specs=pl.BlockSpec((chips, step, HEAD_DIM), lambda i: (0, i, 0)),
        name="project",
    )(grads, their_grads, w_mine, w_theirs)
    parts = lax.all_to_all(partial, "head", 0, 0, axis_index_groups=across, tiled=True)
    summed = pl.pallas_call(
        sum_kernel,
        out_shape=jax.ShapeDtypeStruct((peers, PAGE, HEAD_DIM), half),
        in_specs=[SMEM, VMEM],
        out_specs=VMEM,
        name="sum",
    )(source, parts)
    returned = lax.all_to_all(summed, "tok", 0, 0, tiled=True)
    return pl.pallas_call(
        unpack_kernel,
        out_shape=jax.ShapeDtypeStruct((tok_rows, HEAD_DIM), half),
        in_specs=[SMEM, VMEM],
        out_specs=VMEM,
        name="unpack",
    )(dest, returned)


def solution(mesh):
    placed = (
        P("tok", "head"),
        P("tok", "head"),
        P("tok", "head"),
        P("tok", "head"),
        P(None, "head"),
        P(None, "head"),
        P(None, "head"),
        P("head", None),
        P(),
    )
    return jax.shard_map(
        per_device, mesh=mesh, in_specs=placed, out_specs=P("tok", "head"), check_vma=False
    )
```

```python
import math

import jax
import jax.numpy as jnp
from jax import lax
from jax.experimental import pallas as pl
from jax.experimental.pallas import tpu as pltpu
from jax.sharding import PartitionSpec as P


HEAD_DIM = 128
PAGE = 32
SLOTS = 32
BLOCK = 256
NEG = -1e30
VMEM = pl.BlockSpec(memory_space=pltpu.VMEM)
SMEM = pl.BlockSpec(memory_space=pltpu.SMEM)


def mm(a, b, dims):
    return lax.dot_general(a, b, (dims, ((), ())), preferred_element_type=jnp.float32)


def pack_kernel(dest, query, key, value, sent):
    for page in range(dest.shape[0]):
        peer = dest[page]
        for part, array in enumerate((query, key, value)):
            sent[peer, part * PAGE : (part + 1) * PAGE] = array[page * PAGE : (page + 1) * PAGE]


def grad_kernel(place, here, mine, theirs, w_out, *refs):
    outs, grad, pages = refs[:-2], refs[-2], refs[-1]
    count = mine.shape[0]
    total = None
    for step in range(count):
        chip = lax.rem(here[0] - step + count, count)
        for got, side in ((mine, here[1]), (theirs, 1 - here[1])):
            part = mm(got[step], w_out[2 * chip + side], ((1,), (0,)))
            total = part if total is None else total + part
    grad[...] = total.astype(grad.dtype)
    for page in range(place.shape[0]):
        pages[place[page]] = grad[page * PAGE : (page + 1) * PAGE]
    for step, out in enumerate(outs):
        out[...] = pages[step * out.shape[0] : (step + 1) * out.shape[0]]


def turn_kernel(here, *refs):
    side = len(refs) // 2
    for step, out in enumerate(refs[side:]):
        column = lax.rem(here[0] + step, side)
        for other in range(side):
            out[other] = refs[other][column]


def attention_kernel(source, arrived, *refs):
    side = len(refs) - 8
    turned, grads = refs[:side], refs[side]
    query, key, value, grad, dkey, dvalue, pages = refs[side + 1 :]
    scale = HEAD_DIM ** (-0.5)
    for step, ref in enumerate(turned):
        pages[step * side : (step + 1) * side] = ref[...]
    for slot in range(source.shape[0]):
        code = source[slot]
        peer, place, live = code & 255, (code >> 8) & 255, code >> 16
        at = slice(slot * PAGE, (slot + 1) * PAGE)
        for part, array in enumerate((query, key, value)):
            array[at] = arrived[peer, part * PAGE : (part + 1) * PAGE]
        page = pages[place].astype(jnp.float32) * live.astype(jnp.float32)
        grad[at] = page.astype(grad.dtype)
    total = query.shape[0]
    block = min(BLOCK, total)
    row_order = lax.broadcasted_iota(jnp.int32, (block, block), 0)
    causal = lax.broadcasted_iota(jnp.int32, (block, block), 1) <= row_order
    for first in range(0, total, block):
        last = first + block
        here = slice(first, last)
        spans = ([slice(0, first)] if first else []) + [here]
        part_query, part_grad = query[here], grad[here]
        score = [mm(part_query, key[span], ((1,), (1,))) for span in spans]
        score[-1] = jnp.where(causal, score[-1], NEG)
        row_max = score[-1].max(axis=1, keepdims=True)
        if first:
            row_max = jnp.maximum(row_max, score[0].max(axis=1, keepdims=True))
        raised = [jnp.exp2((s - row_max) * (scale * math.log2(math.e))) for s in score]
        row_sum = sum(r.sum(axis=1, keepdims=True) for r in raised)
        inverse = 1.0 / row_sum
        weights = [r * inverse for r in raised]
        grad_weights = [mm(part_grad, value[span], ((1,), (1,))) for span in spans]
        row_delta = sum((w * g).sum(axis=1, keepdims=True) for w, g in zip(weights, grad_weights))
        grad_score = [
            (w * (g - row_delta)).astype(jnp.bfloat16) for w, g in zip(weights, grad_weights)
        ]
        dquery = sum(mm(d, key[span], ((1,), (0,))) for d, span in zip(grad_score, spans))
        grads[here, 0:HEAD_DIM] = (dquery * scale).astype(grads.dtype)
        for w, d, span in zip(weights, grad_score, spans):
            more_key = mm(d, part_query, ((0,), (0,)))
            more_value = mm(w.astype(jnp.bfloat16), part_grad, ((0,), (0,)))
            if span is here:
                dkey[span] = more_key
                dvalue[span] = more_value
            else:
                dkey[span] += more_key
                dvalue[span] += more_value
    grads[:, HEAD_DIM : 2 * HEAD_DIM] = (dkey[...] * scale).astype(grads.dtype)
    grads[:, 2 * HEAD_DIM : 3 * HEAD_DIM] = dvalue[...].astype(grads.dtype)


def project_kernel(mine, theirs, w_mine, w_theirs, out):
    total = mm(mine[...], w_mine[...], ((1,), (0,))) + mm(theirs[...], w_theirs[...], ((1,), (0,)))
    for x in range(out.shape[0]):
        out[x] = total[:, x * HEAD_DIM : (x + 1) * HEAD_DIM].astype(out.dtype)


def sum_kernel(source, parts, sent):
    for slot in reversed(range(source.shape[0])):
        at = slice(slot * PAGE, (slot + 1) * PAGE)
        total = parts[0, at].astype(jnp.float32)
        for x in range(1, parts.shape[0]):
            total = total + parts[x, at].astype(jnp.float32)
        sent[source[slot] & 255] = total.astype(sent.dtype)


def unpack_kernel(dest, returned, out):
    for page in range(dest.shape[0]):
        out[page * PAGE : (page + 1) * PAGE] = returned[dest[page]]


def per_device(queries, keys, values, out_grad, w_query, w_key, w_value, w_out, page_cluster):
    tok_rows = queries.shape[0]
    pages_here = tok_rows // PAGE
    peers = lax.axis_size("tok")
    heads = lax.axis_size("head")
    chips = heads // 2
    side = math.isqrt(peers)
    myself = lax.axis_index("tok")
    my_z, my_y = myself // side, myself % side
    core = lax.axis_index("head") % 2
    chip = lax.axis_index("head") // 2
    across = [[2 * x + c for x in range(chips)] for c in range(2)]
    swap = [(h, h ^ 1) for h in range(heads)]
    slot_rows = SLOTS * PAGE
    half = queries.dtype

    gathered = [out_grad]
    for d in range(1, chips):
        pairs = [(h, (h + 2 * d) % heads) for h in range(heads)]
        gathered.append(lax.ppermute(out_grad, "head", pairs))

    table = page_cluster.reshape(peers, pages_here)
    dest = lax.dynamic_index_in_dim(table, myself, 0, keepdims=False)
    place = ((dest // side - my_z) % side) * side + dest % side

    sent = pl.pallas_call(
        pack_kernel,
        out_shape=jax.ShapeDtypeStruct((peers, 3 * PAGE, HEAD_DIM), half),
        in_specs=[SMEM] + [VMEM] * 3,
        out_specs=VMEM,
        name="pack",
    )(dest, queries, keys, values)
    sent, w_query, w_key, w_value, page_cluster = lax.optimization_barrier(
        (sent, w_query, w_key, w_value, page_cluster)
    )
    arrived = lax.all_to_all(sent, "tok", 0, 0, tiled=True)

    table = page_cluster.reshape(peers, pages_here)
    has = jnp.any(table == myself, axis=1).astype(jnp.int32)
    peer_order = jnp.arange(peers, dtype=jnp.int32)
    rank = jnp.sum(jnp.where(peer_order[:, None] < peer_order[None, :], has[:, None], 0), axis=0)
    slot_order = jnp.arange(SLOTS, dtype=jnp.int32)
    first_hit = (rank[None, :] == 0) & (has[None, :] == 1)
    hit = (rank[None, :] == slot_order[:, None]) & (has[None, :] == 1)
    live = (slot_order < jnp.sum(has)).astype(jnp.int32)
    hit = jnp.where(live[:, None] == 1, hit, first_hit)
    where_y = (my_y - peer_order % side) % side
    where_z = (my_z - peer_order // side) % side
    code = peer_order + (where_y * side + where_z) * 256
    source = jnp.sum(jnp.where(hit, code[None, :], 0), axis=1) + live * 65536

    mine = jnp.stack(gathered)
    theirs = lax.ppermute(mine, "head", swap)
    w_blocks = w_out.reshape(HEAD_DIM, heads, HEAD_DIM).transpose(1, 2, 0)
    bundle = jax.ShapeDtypeStruct((side, PAGE, HEAD_DIM), half)
    by_z = pl.pallas_call(
        grad_kernel,
        out_shape=[bundle] * side,
        in_specs=[SMEM, SMEM] + [VMEM] * 3,
        out_specs=[VMEM] * side,
        scratch_shapes=[
            pltpu.VMEM((tok_rows, HEAD_DIM), half),
            pltpu.VMEM((peers, PAGE, HEAD_DIM), half),
        ],
        name="grad",
    )(place, jnp.stack([chip, core]), mine, theirs, w_blocks)
    along_z = [by_z[0]]
    for d in range(1, side):
        pairs = [(s, (s // side + d) % side * side + s % side) for s in range(peers)]
        along_z.append(lax.ppermute(by_z[d], "tok", pairs))
    by_y = pl.pallas_call(
        turn_kernel,
        out_shape=[bundle] * side,
        in_specs=[SMEM] + [VMEM] * side,
        out_specs=[VMEM] * side,
        name="turn",
    )(my_y[None], *along_z)
    turned = [by_y[0]]
    for d in range(1, side):
        pairs = [(s, s // side * side + (s % side + d) % side) for s in range(peers)]
        turned.append(lax.ppermute(by_y[d], "tok", pairs))

    weights = jnp.concatenate([w_query, w_key, w_value], axis=1)
    weights = weights.reshape(chips, 2, HEAD_DIM, 3 * HEAD_DIM)
    w_mine = lax.dynamic_index_in_dim(weights, core, 1, keepdims=False)
    w_away = lax.dynamic_index_in_dim(weights, 1 - core, 1, keepdims=False)
    w_mine = w_mine.reshape(chips * HEAD_DIM, 3 * HEAD_DIM).T
    w_away = w_away.reshape(chips * HEAD_DIM, 3 * HEAD_DIM).T
    w_theirs = lax.ppermute(w_away, "head", swap)
    arrived, w_mine, w_theirs, source, *turned = lax.optimization_barrier(
        (arrived, w_mine, w_theirs, source, *turned)
    )

    grads = pl.pallas_call(
        attention_kernel,
        out_shape=jax.ShapeDtypeStruct((slot_rows, 3 * HEAD_DIM), half),
        in_specs=[SMEM, VMEM] + [VMEM] * side,
        out_specs=VMEM,
        scratch_shapes=[pltpu.VMEM((slot_rows, HEAD_DIM), half)] * 4
        + [pltpu.VMEM((slot_rows, HEAD_DIM), jnp.float32)] * 2
        + [pltpu.VMEM((peers, PAGE, HEAD_DIM), half)],
        name="attention",
    )(source, arrived, *turned)
    their_grads = lax.ppermute(grads, "head", swap)
    step = min(BLOCK, slot_rows)
    row_block = pl.BlockSpec((step, 3 * HEAD_DIM), lambda i: (i, 0))
    w_block = pl.BlockSpec(w_mine.shape, lambda i: (0, 0))
    partial = pl.pallas_call(
        project_kernel,
        out_shape=jax.ShapeDtypeStruct((chips, slot_rows, HEAD_DIM), half),
        grid=(slot_rows // step,),
        in_specs=[row_block, row_block, w_block, w_block],
        out_specs=pl.BlockSpec((chips, step, HEAD_DIM), lambda i: (0, i, 0)),
        name="project",
    )(grads, their_grads, w_mine, w_theirs)
    parts = lax.all_to_all(partial, "head", 0, 0, axis_index_groups=across, tiled=True)
    summed = pl.pallas_call(
        sum_kernel,
        out_shape=jax.ShapeDtypeStruct((peers, PAGE, HEAD_DIM), half),
        in_specs=[SMEM, VMEM],
        out_specs=VMEM,
        name="sum",
    )(source, parts)
    returned = lax.all_to_all(summed, "tok", 0, 0, tiled=True)
    return pl.pallas_call(
        unpack_kernel,
        out_shape=jax.ShapeDtypeStruct((tok_rows, HEAD_DIM), half),
        in_specs=[SMEM, VMEM],
        out_specs=VMEM,
        name="unpack",
    )(dest, returned)


def solution(mesh):
    placed = (
        P("tok", "head"),
        P("tok", "head"),
        P("tok", "head"),
        P("tok", "head"),
        P(None, "head"),
        P(None, "head"),
        P(None, "head"),
        P("head", None),
        P(),
    )
    return jax.shard_map(
        per_device, mesh=mesh, in_specs=placed, out_specs=P("tok", "head"), check_vma=False
    )
```

```python
import math

import jax
import jax.numpy as jnp
from jax import lax
from jax.experimental import pallas as pl
from jax.experimental.pallas import tpu as pltpu
from jax.sharding import PartitionSpec as P

HEAD_DIM = 128
PAGE = 32
SLOTS = 32
BLOCK = 256
NEG = -1e30
VMEM = pl.BlockSpec(memory_space=pltpu.VMEM)
SMEM = pl.BlockSpec(memory_space=pltpu.SMEM)


def mm(a, b, dims):
    return lax.dot_general(a, b, (dims, ((), ())), preferred_element_type=jnp.float32)


def small(mib):
    return pltpu.CompilerParams(vmem_limit_bytes=mib * 1024 * 1024)


def pack_kernel(dest, core, query, key, value, even, odd, w_out, sent, grad):
    count = even.shape[0]
    total = None
    for x in range(count):
        for got, side in ((even, core[0]), (odd, 1 - core[0])):
            part = mm(got[x], w_out[2 * x + side], ((1,), (0,)))
            total = part if total is None else total + part
    grad[...] = total.astype(grad.dtype)
    for page in range(dest.shape[0]):
        peer = dest[page]
        for part, array in enumerate((query, key, value, grad)):
            sent[peer, part * PAGE : (part + 1) * PAGE] = array[page * PAGE : (page + 1) * PAGE]


def attention_kernel(source, arrived, grads, query, key, value, grad, dkey, dvalue):
    scale = HEAD_DIM ** (-0.5)
    for slot in range(source.shape[0]):
        peer, live = source[slot] & 255, source[slot] >> 8
        at = slice(slot * PAGE, (slot + 1) * PAGE)
        for part, array in enumerate((query, key, value)):
            array[at] = arrived[peer, part * PAGE : (part + 1) * PAGE]
        page = arrived[peer, 3 * PAGE : 4 * PAGE].astype(jnp.float32) * live.astype(jnp.float32)
        grad[at] = page.astype(grad.dtype)
    total = query.shape[0]
    block = min(BLOCK, total)
    row_order = lax.broadcasted_iota(jnp.int32, (block, block), 0)
    causal = lax.broadcasted_iota(jnp.int32, (block, block), 1) <= row_order
    for first in range(0, total, block):
        last = first + block
        here = slice(first, last)
        spans = ([slice(0, first)] if first else []) + [here]
        part_query, part_grad = query[here], grad[here]
        score = [mm(part_query, key[span], ((1,), (1,))) for span in spans]
        score[-1] = jnp.where(causal, score[-1], NEG)
        row_max = score[-1].max(axis=1, keepdims=True)
        if first:
            row_max = jnp.maximum(row_max, score[0].max(axis=1, keepdims=True))
        raised = [jnp.exp2((s - row_max) * (scale * math.log2(math.e))) for s in score]
        row_sum = sum(r.sum(axis=1, keepdims=True) for r in raised)
        inverse = 1.0 / row_sum
        weights = [r * inverse for r in raised]
        grad_weights = [mm(part_grad, value[span], ((1,), (1,))) for span in spans]
        row_delta = sum((w * g).sum(axis=1, keepdims=True) for w, g in zip(weights, grad_weights))
        grad_score = [
            (w * (g - row_delta)).astype(jnp.bfloat16) for w, g in zip(weights, grad_weights)
        ]
        dquery = sum(mm(d, key[span], ((1,), (0,))) for d, span in zip(grad_score, spans))
        grads[here, 0:HEAD_DIM] = (dquery * scale).astype(grads.dtype)
        for w, d, span in zip(weights, grad_score, spans):
            more_key = mm(d, part_query, ((0,), (0,)))
            more_value = mm(w.astype(jnp.bfloat16), part_grad, ((0,), (0,)))
            if span is here:
                dkey[span] = more_key
                dvalue[span] = more_value
            else:
                dkey[span] += more_key
                dvalue[span] += more_value
    grads[:, HEAD_DIM : 2 * HEAD_DIM] = (dkey[...] * scale).astype(grads.dtype)
    grads[:, 2 * HEAD_DIM : 3 * HEAD_DIM] = dvalue[...].astype(grads.dtype)


def project_kernel(mine, theirs, w_mine, w_theirs, out):
    total_rows = mine.shape[0]
    step = min(BLOCK, total_rows)
    for first in range(0, total_rows, step):
        here = slice(first, first + step)
        for x in range(out.shape[0]):
            cols = slice(x * HEAD_DIM, (x + 1) * HEAD_DIM)
            total = mm(mine[here], w_mine[:, cols], ((1,), (0,)))
            total += mm(theirs[here], w_theirs[:, cols], ((1,), (0,)))
            out[x, here] = total.astype(out.dtype)


def sum_kernel(source, parts, sent):
    for slot in reversed(range(source.shape[0])):
        at = slice(slot * PAGE, (slot + 1) * PAGE)
        total = parts[0, at].astype(jnp.float32)
        for x in range(1, parts.shape[0]):
            total = total + parts[x, at].astype(jnp.float32)
        sent[source[slot] & 255] = total.astype(sent.dtype)


def unpack_kernel(dest, returned, out):
    for page in range(dest.shape[0]):
        out[page * PAGE : (page + 1) * PAGE] = returned[dest[page]]


def per_device(queries, keys, values, out_grad, w_query, w_key, w_value, w_out, page_cluster):
    tok_rows = queries.shape[0]
    pages_here = tok_rows // PAGE
    peers = lax.axis_size("tok")
    heads = lax.axis_size("head")
    chips = heads // 2
    myself = lax.axis_index("tok")
    core = lax.axis_index("head") % 2
    across = [[2 * x + side for x in range(chips)] for side in range(2)]
    swap = [(h, h ^ 1) for h in range(heads)]
    slot_rows = SLOTS * PAGE
    half = queries.dtype

    table = page_cluster.reshape(peers, pages_here)
    dest = lax.dynamic_index_in_dim(table, myself, 0, keepdims=False)
    w_blocks = w_out.reshape(HEAD_DIM, heads, HEAD_DIM).transpose(1, 2, 0)

    same_core = lax.all_to_all(
        jnp.broadcast_to(out_grad[None], (chips, *out_grad.shape)),
        "head", 0, 0, axis_index_groups=across, tiled=True,
    )
    other_core = lax.ppermute(same_core, "head", swap)
    sent = pl.pallas_call(
        pack_kernel,
        out_shape=jax.ShapeDtypeStruct((peers, 4 * PAGE, HEAD_DIM), half),
        in_specs=[SMEM, SMEM] + [VMEM] * 6,
        out_specs=VMEM,
        scratch_shapes=[pltpu.VMEM((tok_rows, HEAD_DIM), half)],
        compiler_params=small(12),
        name="pack",
    )(dest, core[None], queries, keys, values, same_core, other_core, w_blocks)
    sent, w_query, w_key, w_value, page_cluster = lax.optimization_barrier(
        (sent, w_query, w_key, w_value, page_cluster)
    )
    arrived = lax.all_to_all(sent, "tok", 0, 0, tiled=True)
    table = page_cluster.reshape(peers, pages_here)
    has = jnp.any(table == myself, axis=1).astype(jnp.int32)
    peer_order = jnp.arange(peers, dtype=jnp.int32)
    rank = jnp.sum(jnp.where(peer_order[:, None] < peer_order[None, :], has[:, None], 0), axis=0)
    slot_order = jnp.arange(SLOTS, dtype=jnp.int32)
    live = (slot_order < jnp.sum(has)).astype(jnp.int32)
    wanted = jnp.where(live == 1, slot_order, 0)
    hit = (rank[None, :] == wanted[:, None]) & (has[None, :] == 1)
    source = jnp.sum(jnp.where(hit, peer_order[None, :], 0), axis=1) + live * 256
    weights = jnp.concatenate([w_query, w_key, w_value], axis=1)
    weights = weights.reshape(chips, 2, HEAD_DIM, 3 * HEAD_DIM)
    w_mine = lax.dynamic_index_in_dim(weights, core, 1, keepdims=False)
    w_away = lax.dynamic_index_in_dim(weights, 1 - core, 1, keepdims=False)
    w_mine = w_mine.reshape(chips * HEAD_DIM, 3 * HEAD_DIM).T
    w_away = w_away.reshape(chips * HEAD_DIM, 3 * HEAD_DIM).T
    w_theirs = lax.ppermute(w_away, "head", swap)
    arrived, w_mine, w_theirs, source = lax.optimization_barrier(
        (arrived, w_mine, w_theirs, source)
    )
    grads = pl.pallas_call(
        attention_kernel,
        out_shape=jax.ShapeDtypeStruct((slot_rows, 3 * HEAD_DIM), half),
        in_specs=[SMEM, VMEM],
        out_specs=VMEM,
        scratch_shapes=[pltpu.VMEM((slot_rows, HEAD_DIM), half)] * 4
        + [pltpu.VMEM((slot_rows, HEAD_DIM), jnp.float32)] * 2,
        compiler_params=small(24),
        name="attention",
    )(source, arrived)
    their_grads = lax.ppermute(grads, "head", swap)
    partial = pl.pallas_call(
        project_kernel,
        out_shape=jax.ShapeDtypeStruct((chips, slot_rows, HEAD_DIM), half),
        in_specs=[VMEM] * 4,
        out_specs=VMEM,
        compiler_params=small(12),
        name="project",
    )(grads, their_grads, w_mine, w_theirs)
    parts = lax.all_to_all(partial, "head", 0, 0, axis_index_groups=across, tiled=True)
    summed = pl.pallas_call(
        sum_kernel,
        out_shape=jax.ShapeDtypeStruct((peers, PAGE, HEAD_DIM), half),
        in_specs=[SMEM, VMEM],
        out_specs=VMEM,
        compiler_params=small(8),
        name="sum",
    )(source, parts)
    returned = lax.all_to_all(summed, "tok", 0, 0, tiled=True)
    return pl.pallas_call(
        unpack_kernel,
        out_shape=jax.ShapeDtypeStruct((tok_rows, HEAD_DIM), half),
        in_specs=[SMEM, VMEM],
        out_specs=VMEM,
        compiler_params=small(8),
        name="unpack",
    )(dest, returned)


def solution(mesh):
    placed = (
        P("tok", "head"),
        P("tok", "head"),
        P("tok", "head"),
        P("tok", "head"),
        P(None, "head"),
        P(None, "head"),
        P(None, "head"),
        P("head", None),
        P(),
    )
    return jax.shard_map(
        per_device, mesh=mesh, in_specs=placed, out_specs=P("tok", "head"), check_vma=False
    )
```

```python
import math

import jax
import jax.numpy as jnp
from jax import lax
from jax.experimental import pallas as pl
from jax.experimental.pallas import tpu as pltpu
from jax.sharding import PartitionSpec as P


HEAD_DIM = 128
PAGE = 32
SLOTS = 32
BLOCK = 256
NEG = -1e30
VMEM = pl.BlockSpec(memory_space=pltpu.VMEM)
SMEM = pl.BlockSpec(memory_space=pltpu.SMEM)


def mm(a, b, dims):
    return lax.dot_general(a, b, (dims, ((), ())), preferred_element_type=jnp.float32)


def small(mib):
    return pltpu.CompilerParams(vmem_limit_bytes=mib * 1024 * 1024)


def pack_kernel(dest, query, key, value, sent, done):
    copies = []
    for page in range(dest.shape[0]):
        peer = dest[page]
        for part, array in enumerate((query, key, value)):
            copy = pltpu.make_async_copy(
                array.at[pl.ds(page * PAGE, PAGE)],
                sent.at[peer, pl.ds(part * PAGE, PAGE)],
                done.at[page * 3 + part],
            )
            copy.start()
            copies.append(copy)
    for copy in copies:
        copy.wait()


def grad_kernel(dest, here, *refs):
    count = len(refs) - 4
    mine, (theirs, w_out, sent, grad) = refs[:count], refs[count:]
    total = None
    for step in range(count):
        chip = lax.rem(here[0] - step + count, count)
        for got, side in ((mine[step][...], here[1]), (theirs[step], 1 - here[1])):
            part = mm(got, w_out[2 * chip + side], ((1,), (0,)))
            total = part if total is None else total + part
    grad[...] = total.astype(grad.dtype)
    for page in range(dest.shape[0]):
        sent[dest[page]] = grad[page * PAGE : (page + 1) * PAGE]


def spans_of(total):
    block = min(BLOCK, total)
    for first in range(0, total, block):
        here = slice(first, first + block)
        yield here, ([slice(0, first)] if first else []) + [here]


def softmax_of(query, key, here, spans):
    score = [mm(query[here], key[span], ((1,), (1,))) for span in spans]
    row_order = lax.broadcasted_iota(jnp.int32, score[-1].shape, 0)
    causal = lax.broadcasted_iota(jnp.int32, score[-1].shape, 1) <= row_order
    score[-1] = jnp.where(causal, score[-1], NEG)
    row_max = score[-1].max(axis=1, keepdims=True)
    if len(spans) > 1:
        row_max = jnp.maximum(row_max, score[0].max(axis=1, keepdims=True))
    factor = HEAD_DIM ** (-0.5) * math.log2(math.e)
    raised = [jnp.exp2((s - row_max) * factor) for s in score]
    inverse = 1.0 / sum(r.sum(axis=1, keepdims=True) for r in raised)
    return [r * inverse for r in raised]


def weights_kernel(source, arrived, query, key, value, weights):
    for slot in range(source.shape[0]):
        peer = source[slot] & 255
        at = slice(slot * PAGE, (slot + 1) * PAGE)
        for part, array in enumerate((query, key, value)):
            array[at] = arrived[peer, part * PAGE : (part + 1) * PAGE]
    here, spans = list(spans_of(query.shape[0]))[-1]
    for part, span in zip(softmax_of(query, key, here, spans), spans):
        weights[:, span] = part


def attention_kernel(
    source, query, key, value, weights, arrived, grads, grad, dkey, dvalue
):
    scale = HEAD_DIM ** (-0.5)
    for slot in range(source.shape[0]):
        peer, live = source[slot] & 255, source[slot] >> 8
        at = slice(slot * PAGE, (slot + 1) * PAGE)
        page = arrived[peer].astype(jnp.float32) * live.astype(jnp.float32)
        grad[at] = page.astype(grad.dtype)
    for here, spans in spans_of(query.shape[0]):
        part_query, part_grad = query[here], grad[here]
        if here.stop == query.shape[0]:
            part_weights = [weights[:, span] for span in spans]
        else:
            part_weights = softmax_of(query, key, here, spans)
        grad_weights = [mm(part_grad, value[span], ((1,), (1,))) for span in spans]
        row_delta = sum(
            (w * g).sum(axis=1, keepdims=True) for w, g in zip(part_weights, grad_weights)
        )
        grad_score = [
            (w * (g - row_delta)).astype(jnp.bfloat16)
            for w, g in zip(part_weights, grad_weights)
        ]
        dquery = sum(mm(d, key[span], ((1,), (0,))) for d, span in zip(grad_score, spans))
        grads[here, 0:HEAD_DIM] = (dquery * scale).astype(grads.dtype)
        for w, d, span in zip(part_weights, grad_score, spans):
            more_key = mm(d, part_query, ((0,), (0,)))
            more_value = mm(w.astype(jnp.bfloat16), part_grad, ((0,), (0,)))
            if span is here:
                dkey[span] = more_key
                dvalue[span] = more_value
            else:
                dkey[span] += more_key
                dvalue[span] += more_value
    grads[:, HEAD_DIM : 2 * HEAD_DIM] = (dkey[...] * scale).astype(grads.dtype)
    grads[:, 2 * HEAD_DIM : 3 * HEAD_DIM] = dvalue[...].astype(grads.dtype)


def project_kernel(*refs):
    grads, weights, out = refs[-3:]
    total_rows = grads.shape[0]
    step = min(BLOCK, total_rows)
    for first in range(0, total_rows, step):
        here = slice(first, first + step)
        for x in range(out.shape[0]):
            cols = slice(x * HEAD_DIM, (x + 1) * HEAD_DIM)
            total = mm(grads[here], weights[:, cols], ((1,), (0,)))
            if len(refs) > 3:
                total += refs[0][x, here]
            out[x, here] = total.astype(out.dtype)


def sum_kernel(source, parts, sent):
    for slot in reversed(range(source.shape[0])):
        at = slice(slot * PAGE, (slot + 1) * PAGE)
        total = parts[0, at].astype(jnp.float32)
        for x in range(1, parts.shape[0]):
            total = total + parts[x, at].astype(jnp.float32)
        sent[source[slot] & 255] = total.astype(sent.dtype)


def unpack_kernel(dest, returned, out):
    for page in range(dest.shape[0]):
        out[page * PAGE : (page + 1) * PAGE] = returned[dest[page]]


def per_device(queries, keys, values, out_grad, w_query, w_key, w_value, w_out, page_cluster):
    tok_rows = queries.shape[0]
    pages_here = tok_rows // PAGE
    peers = lax.axis_size("tok")
    heads = lax.axis_size("head")
    chips = heads // 2
    myself = lax.axis_index("tok")
    core = lax.axis_index("head") % 2
    chip = lax.axis_index("head") // 2
    across = [[2 * x + c for x in range(chips)] for c in range(2)]
    swap = [(h, h ^ 1) for h in range(heads)]
    slot_rows = SLOTS * PAGE
    half = queries.dtype

    def moved(array, pairs):
        return lax.ppermute(array, "head", pairs)

    def work(products, moved_bytes):
        return pl.CostEstimate(flops=2 * products, bytes_accessed=moved_bytes, transcendentals=0)

    table = page_cluster.reshape(peers, pages_here)
    dest = lax.dynamic_index_in_dim(table, myself, 0, keepdims=False)
    sent = pl.pallas_call(
        pack_kernel,
        out_shape=jax.ShapeDtypeStruct((peers, 3 * PAGE, HEAD_DIM), half),
        in_specs=[SMEM] + [VMEM] * 3,
        out_specs=pl.BlockSpec(memory_space=pl.ANY),
        scratch_shapes=[pltpu.SemaphoreType.DMA((3 * pages_here,))],
        compiler_params=small(8),
        name="pack",
    )(dest, queries, keys, values)
    sent, w_query, w_key, w_value, page_cluster = lax.optimization_barrier(
        (sent, w_query, w_key, w_value, page_cluster)
    )
    arrived = lax.all_to_all(sent, "tok", 0, 0, tiled=True)

    gathered = [out_grad]
    for d in range(1, chips):
        pairs = [(h, (h + 2 * d) % heads) for h in range(heads)]
        gathered.append(moved(out_grad, pairs))
    theirs = moved(jnp.stack(gathered), swap)
    w_blocks = w_out.reshape(HEAD_DIM, heads, HEAD_DIM).transpose(1, 2, 0)
    sent_grad = pl.pallas_call(
        grad_kernel,
        out_shape=jax.ShapeDtypeStruct((peers, PAGE, HEAD_DIM), half),
        in_specs=[SMEM, SMEM] + [VMEM] * (chips + 2),
        out_specs=VMEM,
        scratch_shapes=[pltpu.VMEM((tok_rows, HEAD_DIM), half)],
        compiler_params=small(12),
        cost_estimate=work(tok_rows * heads * HEAD_DIM**2, 4 * tok_rows * heads * HEAD_DIM),
        name="grad",
    )(dest, jnp.stack([chip, core]), *gathered, theirs, w_blocks)
    table = page_cluster.reshape(peers, pages_here)
    has = jnp.any(table == myself, axis=1).astype(jnp.int32)
    peer_order = jnp.arange(peers, dtype=jnp.int32)
    rank = jnp.sum(jnp.where(peer_order[:, None] < peer_order[None, :], has[:, None], 0), axis=0)
    slot_order = jnp.arange(SLOTS, dtype=jnp.int32)
    live = (slot_order < jnp.sum(has)).astype(jnp.int32)
    wanted = jnp.where(live == 1, slot_order, 0)
    hit = (rank[None, :] == wanted[:, None]) & (has[None, :] == 1)
    source = jnp.sum(jnp.where(hit, peer_order[None, :], 0), axis=1) + live * 256
    weights = jnp.concatenate([w_query, w_key, w_value], axis=1)
    weights = weights.reshape(chips, 2, HEAD_DIM, 3 * HEAD_DIM)
    w_mine = lax.dynamic_index_in_dim(weights, core, 1, keepdims=False)
    w_away = lax.dynamic_index_in_dim(weights, 1 - core, 1, keepdims=False)
    w_mine = w_mine.reshape(chips * HEAD_DIM, 3 * HEAD_DIM).T
    w_away = w_away.reshape(chips * HEAD_DIM, 3 * HEAD_DIM).T
    w_theirs = moved(w_away, swap)
    arrived, w_mine, w_theirs, source, sent_grad = lax.optimization_barrier(
        (arrived, w_mine, w_theirs, source, sent_grad)
    )
    arrived_grad = lax.all_to_all(sent_grad, "tok", 0, 0, tiled=True)
    flat = jax.ShapeDtypeStruct((slot_rows, HEAD_DIM), half)
    *paged, weighted = pl.pallas_call(
        weights_kernel,
        out_shape=[flat] * 3
        + [jax.ShapeDtypeStruct((min(BLOCK, slot_rows), slot_rows), jnp.float32)],
        in_specs=[SMEM, VMEM],
        out_specs=[VMEM] * 4,
        compiler_params=small(24),
        cost_estimate=work(BLOCK * slot_rows * HEAD_DIM, 4 * BLOCK * slot_rows),
        name="softmax",
    )(source, arrived)
    grads = pl.pallas_call(
        attention_kernel,
        out_shape=jax.ShapeDtypeStruct((slot_rows, 3 * HEAD_DIM), half),
        in_specs=[SMEM] + [VMEM] * 5,
        out_specs=VMEM,
        scratch_shapes=[pltpu.VMEM((slot_rows, HEAD_DIM), half)]
        + [pltpu.VMEM((slot_rows, HEAD_DIM), jnp.float32)] * 2,
        compiler_params=small(24),
        cost_estimate=work(3 * slot_rows**2 * HEAD_DIM, 4 * slot_rows**2),
        name="attention",
    )(source, *paged, weighted, arrived_grad)

    def projected(*arrays, dtype):
        return pl.pallas_call(
            project_kernel,
            out_shape=jax.ShapeDtypeStruct((chips, slot_rows, HEAD_DIM), dtype),
            in_specs=[VMEM] * len(arrays),
            out_specs=VMEM,
            compiler_params=small(16),
            cost_estimate=work(slot_rows * w_mine.size, 8 * slot_rows * w_mine.shape[1]),
        )(*arrays)

    their_grads = moved(grads, swap)
    partial = projected(grads, w_mine, dtype=jnp.float32)
    partial = projected(partial, their_grads, w_theirs, dtype=half)
    parts = lax.all_to_all(partial, "head", 0, 0, axis_index_groups=across, tiled=True)
    summed = pl.pallas_call(
        sum_kernel,
        out_shape=jax.ShapeDtypeStruct((peers, PAGE, HEAD_DIM), half),
        in_specs=[SMEM, VMEM],
        out_specs=VMEM,
        compiler_params=small(8),
        name="sum",
    )(source, parts)
    returned = lax.all_to_all(summed, "tok", 0, 0, tiled=True)
    return pl.pallas_call(
        unpack_kernel,
        out_shape=jax.ShapeDtypeStruct((tok_rows, HEAD_DIM), half),
        in_specs=[SMEM, VMEM],
        out_specs=VMEM,
        compiler_params=small(8),
        name="unpack",
    )(dest, returned)


def solution(mesh):
    placed = (
        P("tok", "head"),
        P("tok", "head"),
        P("tok", "head"),
        P("tok", "head"),
        P(None, "head"),
        P(None, "head"),
        P(None, "head"),
        P("head", None),
        P(),
    )
    return jax.shard_map(
        per_device, mesh=mesh, in_specs=placed, out_specs=P("tok", "head"), check_vma=False
    )
```

```python
import math

import jax
import jax.numpy as jnp
from jax import lax
from jax.experimental import pallas as pl
from jax.experimental.pallas import tpu as pltpu
from jax.sharding import PartitionSpec as P


HEAD_DIM = 128
PAGE = 32
SLOTS = 32
BLOCK = 256
NEG = -1e30
VMEM = pl.BlockSpec(memory_space=pltpu.VMEM)
SMEM = pl.BlockSpec(memory_space=pltpu.SMEM)


def mm(a, b, dims):
    return lax.dot_general(a, b, (dims, ((), ())), preferred_element_type=jnp.float32)


def small(mib):
    return pltpu.CompilerParams(vmem_limit_bytes=mib * 1024 * 1024)


def pack_kernel(table, query, key, value, sent, done):
    copies = []
    pages = query.shape[0] // PAGE
    first = lax.axis_index("tok") * pages
    for page in range(pages):
        peer = table[first + page]
        for part, array in enumerate((query, key, value)):
            copy = pltpu.make_async_copy(
                array.at[pl.ds(page * PAGE, PAGE)],
                sent.at[peer, pl.ds(part * PAGE, PAGE)],
                done.at[page * 3 + part],
            )
            copy.start()
            copies.append(copy)
    for copy in copies:
        copy.wait()


def grad_kernel(dest, here, *refs):
    count = len(refs) - 4
    mine, (theirs, w_out, sent, grad) = refs[:count], refs[count:]
    total = None
    for step in range(count):
        chip = lax.rem(here[0] - step + count, count)
        for got, side in ((mine[step][...], here[1]), (theirs[step], 1 - here[1])):
            part = mm(got, w_out[2 * chip + side], ((1,), (0,)))
            total = part if total is None else total + part
    grad[...] = total.astype(grad.dtype)
    for page in range(dest.shape[0]):
        sent[dest[page]] = grad[page * PAGE : (page + 1) * PAGE]


def spans_of(total):
    block = min(BLOCK, total)
    for first in range(0, total, block):
        here = slice(first, first + block)
        yield here, ([slice(0, first)] if first else []) + [here]


def softmax_of(query, key, here, spans):
    score = [mm(query[here], key[span], ((1,), (1,))) for span in spans]
    row_order = lax.broadcasted_iota(jnp.int32, score[-1].shape, 0)
    causal = lax.broadcasted_iota(jnp.int32, score[-1].shape, 1) <= row_order
    score[-1] = jnp.where(causal, score[-1], NEG)
    row_max = score[-1].max(axis=1, keepdims=True)
    if len(spans) > 1:
        row_max = jnp.maximum(row_max, score[0].max(axis=1, keepdims=True))
    factor = HEAD_DIM ** (-0.5) * math.log2(math.e)
    raised = [jnp.exp2((s - row_max) * factor) for s in score]
    inverse = 1.0 / sum(r.sum(axis=1, keepdims=True) for r in raised)
    return [r * inverse for r in raised]


def assemble_kernel(source, arrived, paged):
    for slot in range(source.shape[0]):
        peer = source[slot] & 255
        at = slice(slot * PAGE, (slot + 1) * PAGE)
        for part in range(3):
            paged[part, at] = arrived[peer, part * PAGE : (part + 1) * PAGE]


def attention_kernel(source, paged, arrived, grads, grad, dkey, dvalue):
    query, key, value = paged.at[0], paged.at[1], paged.at[2]
    scale = HEAD_DIM ** (-0.5)
    for slot in range(source.shape[0]):
        peer, live = source[slot] & 255, source[slot] >> 8
        at = slice(slot * PAGE, (slot + 1) * PAGE)
        page = arrived[peer].astype(jnp.float32) * live.astype(jnp.float32)
        grad[at] = page.astype(grad.dtype)
    for here, spans in spans_of(query.shape[0]):
        part_query, part_grad = query[here], grad[here]
        part_weights = softmax_of(query, key, here, spans)
        grad_weights = [mm(part_grad, value[span], ((1,), (1,))) for span in spans]
        row_delta = sum(
            (w * g).sum(axis=1, keepdims=True) for w, g in zip(part_weights, grad_weights)
        )
        grad_score = [
            (w * (g - row_delta)).astype(jnp.bfloat16)
            for w, g in zip(part_weights, grad_weights)
        ]
        dquery = sum(mm(d, key[span], ((1,), (0,))) for d, span in zip(grad_score, spans))
        grads[here, 0:HEAD_DIM] = (dquery * scale).astype(grads.dtype)
        for w, d, span in zip(part_weights, grad_score, spans):
            more_key = mm(d, part_query, ((0,), (0,)))
            more_value = mm(w.astype(jnp.bfloat16), part_grad, ((0,), (0,)))
            if span is here:
                dkey[span] = more_key
                dvalue[span] = more_value
            else:
                dkey[span] += more_key
                dvalue[span] += more_value
    grads[:, HEAD_DIM : 2 * HEAD_DIM] = (dkey[...] * scale).astype(grads.dtype)
    grads[:, 2 * HEAD_DIM : 3 * HEAD_DIM] = dvalue[...].astype(grads.dtype)


def project_kernel(*refs):
    grads, weights, out = refs[-3:]
    total_rows = grads.shape[0]
    step = min(BLOCK, total_rows)
    for first in range(0, total_rows, step):
        here = slice(first, first + step)
        for x in range(out.shape[0]):
            cols = slice(x * HEAD_DIM, (x + 1) * HEAD_DIM)
            total = mm(grads[here], weights[:, cols], ((1,), (0,)))
            if len(refs) > 3:
                total += refs[0][x, here]
            out[x, here] = total.astype(out.dtype)


def sum_kernel(source, parts, sent):
    for slot in reversed(range(source.shape[0])):
        at = slice(slot * PAGE, (slot + 1) * PAGE)
        total = parts[0, at].astype(jnp.float32)
        for x in range(1, parts.shape[0]):
            total = total + parts[x, at].astype(jnp.float32)
        sent[source[slot] & 255] = total.astype(sent.dtype)


def unpack_kernel(dest, returned, out):
    for page in range(dest.shape[0]):
        out[page * PAGE : (page + 1) * PAGE] = returned[dest[page]]


def per_device(queries, keys, values, out_grad, w_query, w_key, w_value, w_out, page_cluster):
    tok_rows = queries.shape[0]
    pages_here = tok_rows // PAGE
    peers = lax.axis_size("tok")
    heads = lax.axis_size("head")
    chips = heads // 2
    myself = lax.axis_index("tok")
    core = lax.axis_index("head") % 2
    chip = lax.axis_index("head") // 2
    across = [[2 * x + c for x in range(chips)] for c in range(2)]
    swap = [(h, h ^ 1) for h in range(heads)]
    slot_rows = SLOTS * PAGE
    half = queries.dtype

    def moved(array, pairs):
        return lax.ppermute(array, "head", pairs)

    def work(products, moved_bytes):
        return pl.CostEstimate(flops=2 * products, bytes_accessed=moved_bytes, transcendentals=0)

    sent = pl.pallas_call(
        pack_kernel,
        out_shape=jax.ShapeDtypeStruct((peers, 3 * PAGE, HEAD_DIM), half),
        in_specs=[SMEM] + [VMEM] * 3,
        out_specs=pl.BlockSpec(memory_space=pl.ANY),
        scratch_shapes=[pltpu.SemaphoreType.DMA((3 * pages_here,))],
        name="pack",
    )(page_cluster, queries, keys, values)
    sent, w_query, w_key, w_value, page_cluster = lax.optimization_barrier(
        (sent, w_query, w_key, w_value, page_cluster)
    )
    arrived = lax.all_to_all(sent, "tok", 0, 0, tiled=True)
    dest = lax.dynamic_slice_in_dim(page_cluster, myself * pages_here, pages_here)

    gathered = [out_grad]
    for d in range(1, chips):
        pairs = [(h, (h + 2 * d) % heads) for h in range(heads)]
        gathered.append(moved(out_grad, pairs))
    theirs = moved(jnp.stack(gathered), swap)
    w_blocks = w_out.reshape(HEAD_DIM, heads, HEAD_DIM).transpose(1, 2, 0)
    sent_grad = pl.pallas_call(
        grad_kernel,
        out_shape=jax.ShapeDtypeStruct((peers, PAGE, HEAD_DIM), half),
        in_specs=[SMEM, SMEM] + [VMEM] * (chips + 2),
        out_specs=VMEM,
        scratch_shapes=[pltpu.VMEM((tok_rows, HEAD_DIM), half)],
        compiler_params=small(12),
        cost_estimate=work(tok_rows * heads * HEAD_DIM**2, 4 * tok_rows * heads * HEAD_DIM),
        name="grad",
    )(dest, jnp.stack([chip, core]), *gathered, theirs, w_blocks)
    table = page_cluster.reshape(peers, pages_here)
    has = jnp.any(table == myself, axis=1).astype(jnp.int32)
    peer_order = jnp.arange(peers, dtype=jnp.int32)
    rank = jnp.sum(jnp.where(peer_order[:, None] < peer_order[None, :], has[:, None], 0), axis=0)
    slot_order = jnp.arange(SLOTS, dtype=jnp.int32)
    live = (slot_order < jnp.sum(has)).astype(jnp.int32)
    wanted = jnp.where(live == 1, slot_order, 0)
    hit = (rank[None, :] == wanted[:, None]) & (has[None, :] == 1)
    source = jnp.sum(jnp.where(hit, peer_order[None, :], 0), axis=1) + live * 256
    weights = jnp.concatenate([w_query, w_key, w_value], axis=1)
    weights = weights.reshape(chips, 2, HEAD_DIM, 3 * HEAD_DIM)
    w_mine = lax.dynamic_index_in_dim(weights, core, 1, keepdims=False)
    w_away = lax.dynamic_index_in_dim(weights, 1 - core, 1, keepdims=False)
    w_mine = w_mine.reshape(chips * HEAD_DIM, 3 * HEAD_DIM).T
    w_away = w_away.reshape(chips * HEAD_DIM, 3 * HEAD_DIM).T
    w_theirs = moved(w_away, swap)
    arrived, w_mine, w_theirs, source, sent_grad = lax.optimization_barrier(
        (arrived, w_mine, w_theirs, source, sent_grad)
    )
    arrived_grad = lax.all_to_all(sent_grad, "tok", 0, 0, tiled=True)
    paged = pl.pallas_call(
        assemble_kernel,
        out_shape=jax.ShapeDtypeStruct((3, slot_rows, HEAD_DIM), half),
        in_specs=[SMEM, VMEM],
        out_specs=VMEM,
        compiler_params=small(8),
        cost_estimate=work(slot_rows**2, 12 * slot_rows * HEAD_DIM),
        name="assemble",
    )(source, arrived)
    grads = pl.pallas_call(
        attention_kernel,
        out_shape=jax.ShapeDtypeStruct((slot_rows, 3 * HEAD_DIM), half),
        in_specs=[SMEM] + [VMEM] * 2,
        out_specs=VMEM,
        scratch_shapes=[pltpu.VMEM((slot_rows, HEAD_DIM), half)]
        + [pltpu.VMEM((slot_rows, HEAD_DIM), jnp.float32)] * 2,
        compiler_params=small(24),
        cost_estimate=work(3 * slot_rows**2 * HEAD_DIM, 4 * slot_rows**2),
        name="attention",
    )(source, paged, arrived_grad)

    def projected(*arrays, dtype):
        return pl.pallas_call(
            project_kernel,
            out_shape=jax.ShapeDtypeStruct((chips, slot_rows, HEAD_DIM), dtype),
            in_specs=[VMEM] * len(arrays),
            out_specs=VMEM,
            compiler_params=small(16),
            cost_estimate=work(slot_rows * w_mine.size, 8 * slot_rows * w_mine.shape[1]),
        )(*arrays)

    their_grads = moved(grads, swap)
    partial = projected(grads, w_mine, dtype=jnp.float32)
    partial = projected(partial, their_grads, w_theirs, dtype=half)
    parts = lax.all_to_all(partial, "head", 0, 0, axis_index_groups=across, tiled=True)
    summed = pl.pallas_call(
        sum_kernel,
        out_shape=jax.ShapeDtypeStruct((peers, PAGE, HEAD_DIM), half),
        in_specs=[SMEM, VMEM],
        out_specs=VMEM,
        compiler_params=small(8),
        name="sum",
    )(source, parts)
    returned = lax.all_to_all(summed, "tok", 0, 0, tiled=True)
    return pl.pallas_call(
        unpack_kernel,
        out_shape=jax.ShapeDtypeStruct((tok_rows, HEAD_DIM), half),
        in_specs=[SMEM, VMEM],
        out_specs=VMEM,
        compiler_params=small(8),
        name="unpack",
    )(dest, returned)


def solution(mesh):
    placed = (
        P("tok", "head"),
        P("tok", "head"),
        P("tok", "head"),
        P("tok", "head"),
        P(None, "head"),
        P(None, "head"),
        P(None, "head"),
        P("head", None),
        P(),
    )
    return jax.shard_map(
        per_device, mesh=mesh, in_specs=placed, out_specs=P("tok", "head"), check_vma=False
    )
```

```python
import math

import jax
import jax.numpy as jnp
from jax import lax
from jax.experimental import pallas as pl
from jax.experimental.pallas import tpu as pltpu
from jax.sharding import PartitionSpec as P


HEAD_DIM = 128
PAGE = 32
SLOTS = 32
BLOCK = 256
NEG = -1e30
VMEM = pl.BlockSpec(memory_space=pltpu.VMEM)
SMEM = pl.BlockSpec(memory_space=pltpu.SMEM)


def mm(a, b, dims):
    return lax.dot_general(a, b, (dims, ((), ())), preferred_element_type=jnp.float32)


def small(mib):
    return pltpu.CompilerParams(vmem_limit_bytes=mib * 1024 * 1024)


def pack_kernel(table, query, key, value, sent, done):
    copies = []
    pages = query.shape[0] // PAGE
    first = lax.axis_index("tok") * pages
    for page in range(pages):
        peer = table[first + page]
        for part, array in enumerate((query, key, value)):
            copy = pltpu.make_async_copy(
                array.at[pl.ds(page * PAGE, PAGE)],
                sent.at[peer, pl.ds(part * PAGE, PAGE)],
                done.at[page * 3 + part],
            )
            copy.start()
            copies.append(copy)
    for copy in copies:
        copy.wait()


def grad_kernel(dest, here, *refs):
    count = len(refs) - 4
    mine, (theirs, w_out, sent, grad) = refs[:count], refs[count:]
    total = None
    for step in range(count):
        chip = lax.rem(here[0] - step + count, count)
        for got, side in ((mine[step][...], here[1]), (theirs[step], 1 - here[1])):
            part = mm(got, w_out[2 * chip + side], ((1,), (0,)))
            total = part if total is None else total + part
    grad[...] = total.astype(grad.dtype)
    for page in range(dest.shape[0]):
        sent[dest[page]] = grad[page * PAGE : (page + 1) * PAGE]


def spans_of(total):
    block = min(BLOCK, total)
    for first in range(0, total, block):
        here = slice(first, first + block)
        yield here, ([slice(0, first)] if first else []) + [here]


def softmax_of(query, key, here, spans):
    score = [mm(key[span], query[here], ((1,), (1,))) for span in spans]
    key_order = lax.broadcasted_iota(jnp.int32, score[-1].shape, 0)
    causal = key_order <= lax.broadcasted_iota(jnp.int32, score[-1].shape, 1)
    score[-1] = jnp.where(causal, score[-1], NEG)
    top = score[-1].max(axis=0, keepdims=True)
    if len(spans) > 1:
        top = jnp.maximum(top, score[0].max(axis=0, keepdims=True))
    factor = HEAD_DIM ** (-0.5) * math.log2(math.e)
    raised = [jnp.exp2((s - top) * factor) for s in score]
    inverse = 1.0 / sum(r.sum(axis=0, keepdims=True) for r in raised)
    return [r * inverse for r in raised]


def assemble_kernel(source, arrived, paged):
    for slot in range(source.shape[0]):
        peer = source[slot] & 255
        at = slice(slot * PAGE, (slot + 1) * PAGE)
        for part in range(3):
            paged[part, at] = arrived[peer, part * PAGE : (part + 1) * PAGE]


def attention_kernel(source, paged, arrived, grads, grad, dkey, dvalue):
    query, key, value = paged.at[0], paged.at[1], paged.at[2]
    scale = HEAD_DIM ** (-0.5)
    for slot in range(source.shape[0]):
        peer, live = source[slot] & 255, source[slot] >> 8
        at = slice(slot * PAGE, (slot + 1) * PAGE)
        page = arrived[peer].astype(jnp.float32) * live.astype(jnp.float32)
        grad[at] = page.astype(grad.dtype)
    for here, spans in spans_of(query.shape[0]):
        part_query, part_grad = query[here], grad[here]
        part_weights = softmax_of(query, key, here, spans)
        grad_weights = [mm(value[span], part_grad, ((1,), (1,))) for span in spans]
        row_delta = sum(
            (w * g).sum(axis=0, keepdims=True) for w, g in zip(part_weights, grad_weights)
        )
        grad_score = [
            (w * (g - row_delta)).astype(jnp.bfloat16)
            for w, g in zip(part_weights, grad_weights)
        ]
        dquery = sum(mm(d, key[span], ((0,), (0,))) for d, span in zip(grad_score, spans))
        grads[here, 0:HEAD_DIM] = (dquery * scale).astype(grads.dtype)
        for w, d, span in zip(part_weights, grad_score, spans):
            more_key = mm(d, part_query, ((1,), (0,)))
            more_value = mm(w.astype(jnp.bfloat16), part_grad, ((1,), (0,)))
            if span is here:
                dkey[span] = more_key
                dvalue[span] = more_value
            else:
                dkey[span] += more_key
                dvalue[span] += more_value
    grads[:, HEAD_DIM : 2 * HEAD_DIM] = (dkey[...] * scale).astype(grads.dtype)
    grads[:, 2 * HEAD_DIM : 3 * HEAD_DIM] = dvalue[...].astype(grads.dtype)


def project_kernel(*refs):
    grads, weights, out = refs[-3:]
    total_rows = grads.shape[0]
    step = min(BLOCK, total_rows)
    for first in range(0, total_rows, step):
        here = slice(first, first + step)
        for x in range(out.shape[0]):
            cols = slice(x * HEAD_DIM, (x + 1) * HEAD_DIM)
            total = mm(grads[here], weights[:, cols], ((1,), (0,)))
            if len(refs) > 3:
                total += refs[0][x, here]
            out[x, here] = total.astype(out.dtype)


def sum_kernel(source, parts, sent):
    for slot in reversed(range(source.shape[0])):
        at = slice(slot * PAGE, (slot + 1) * PAGE)
        total = parts[0, at].astype(jnp.float32)
        for x in range(1, parts.shape[0]):
            total = total + parts[x, at].astype(jnp.float32)
        sent[source[slot] & 255] = total.astype(sent.dtype)


def unpack_kernel(dest, returned, out):
    for page in range(dest.shape[0]):
        out[page * PAGE : (page + 1) * PAGE] = returned[dest[page]]


def per_device(queries, keys, values, out_grad, w_query, w_key, w_value, w_out, page_cluster):
    tok_rows = queries.shape[0]
    pages_here = tok_rows // PAGE
    peers = lax.axis_size("tok")
    heads = lax.axis_size("head")
    chips = heads // 2
    myself = lax.axis_index("tok")
    core = lax.axis_index("head") % 2
    chip = lax.axis_index("head") // 2
    across = [[2 * x + c for x in range(chips)] for c in range(2)]
    swap = [(h, h ^ 1) for h in range(heads)]
    slot_rows = SLOTS * PAGE
    half = queries.dtype

    def moved(array, pairs):
        return lax.ppermute(array, "head", pairs)

    def work(products, moved_bytes):
        return pl.CostEstimate(flops=2 * products, bytes_accessed=moved_bytes, transcendentals=0)

    sent = pl.pallas_call(
        pack_kernel,
        out_shape=jax.ShapeDtypeStruct((peers, 3 * PAGE, HEAD_DIM), half),
        in_specs=[SMEM] + [VMEM] * 3,
        out_specs=pl.BlockSpec(memory_space=pl.ANY),
        scratch_shapes=[pltpu.SemaphoreType.DMA((3 * pages_here,))],
        name="pack",
    )(page_cluster, queries, keys, values)
    sent, w_query, w_key, w_value, page_cluster = lax.optimization_barrier(
        (sent, w_query, w_key, w_value, page_cluster)
    )
    arrived = lax.all_to_all(sent, "tok", 0, 0, tiled=True)
    dest = lax.dynamic_slice_in_dim(page_cluster, myself * pages_here, pages_here)

    gathered = [out_grad]
    for d in range(1, chips):
        pairs = [(h, (h + 2 * d) % heads) for h in range(heads)]
        gathered.append(moved(out_grad, pairs))
    theirs = moved(jnp.stack(gathered), swap)
    w_blocks = w_out.reshape(HEAD_DIM, heads, HEAD_DIM).transpose(1, 2, 0)
    sent_grad = pl.pallas_call(
        grad_kernel,
        out_shape=jax.ShapeDtypeStruct((peers, PAGE, HEAD_DIM), half),
        in_specs=[SMEM, SMEM] + [VMEM] * (chips + 2),
        out_specs=VMEM,
        scratch_shapes=[pltpu.VMEM((tok_rows, HEAD_DIM), half)],
        compiler_params=small(12),
        cost_estimate=work(tok_rows * heads * HEAD_DIM**2, 4 * tok_rows * heads * HEAD_DIM),
        name="grad",
    )(dest, jnp.stack([chip, core]), *gathered, theirs, w_blocks)
    table = page_cluster.reshape(peers, pages_here)
    has = jnp.any(table == myself, axis=1).astype(jnp.int32)
    peer_order = jnp.arange(peers, dtype=jnp.int32)
    rank = jnp.sum(jnp.where(peer_order[:, None] < peer_order[None, :], has[:, None], 0), axis=0)
    slot_order = jnp.arange(SLOTS, dtype=jnp.int32)
    live = (slot_order < jnp.sum(has)).astype(jnp.int32)
    wanted = jnp.where(live == 1, slot_order, 0)
    hit = (rank[None, :] == wanted[:, None]) & (has[None, :] == 1)
    source = jnp.sum(jnp.where(hit, peer_order[None, :], 0), axis=1) + live * 256
    weights = jnp.concatenate([w_query, w_key, w_value], axis=1)
    weights = weights.reshape(chips, 2, HEAD_DIM, 3 * HEAD_DIM)
    w_mine = lax.dynamic_index_in_dim(weights, core, 1, keepdims=False)
    w_away = lax.dynamic_index_in_dim(weights, 1 - core, 1, keepdims=False)
    w_mine = w_mine.reshape(chips * HEAD_DIM, 3 * HEAD_DIM).T
    w_away = w_away.reshape(chips * HEAD_DIM, 3 * HEAD_DIM).T
    w_theirs = moved(w_away, swap)
    arrived, w_mine, w_theirs, source, sent_grad = lax.optimization_barrier(
        (arrived, w_mine, w_theirs, source, sent_grad)
    )
    arrived_grad = lax.all_to_all(sent_grad, "tok", 0, 0, tiled=True)
    paged = pl.pallas_call(
        assemble_kernel,
        out_shape=jax.ShapeDtypeStruct((3, slot_rows, HEAD_DIM), half),
        in_specs=[SMEM, VMEM],
        out_specs=VMEM,
        compiler_params=small(8),
        cost_estimate=work(slot_rows**2, 12 * slot_rows * HEAD_DIM),
        name="assemble",
    )(source, arrived)
    grads = pl.pallas_call(
        attention_kernel,
        out_shape=jax.ShapeDtypeStruct((slot_rows, 3 * HEAD_DIM), half),
        in_specs=[SMEM] + [VMEM] * 2,
        out_specs=VMEM,
        scratch_shapes=[pltpu.VMEM((slot_rows, HEAD_DIM), half)]
        + [pltpu.VMEM((slot_rows, HEAD_DIM), jnp.float32)] * 2,
        compiler_params=small(24),
        cost_estimate=work(3 * slot_rows**2 * HEAD_DIM, 4 * slot_rows**2),
        name="attention",
    )(source, paged, arrived_grad)

    def projected(*arrays, dtype):
        return pl.pallas_call(
            project_kernel,
            out_shape=jax.ShapeDtypeStruct((chips, slot_rows, HEAD_DIM), dtype),
            in_specs=[VMEM] * len(arrays),
            out_specs=VMEM,
            compiler_params=small(16),
            cost_estimate=work(slot_rows * w_mine.size, 8 * slot_rows * w_mine.shape[1]),
        )(*arrays)

    their_grads = moved(grads, swap)
    partial = projected(grads, w_mine, dtype=jnp.float32)
    partial = projected(partial, their_grads, w_theirs, dtype=half)
    parts = lax.all_to_all(partial, "head", 0, 0, axis_index_groups=across, tiled=True)
    summed = pl.pallas_call(
        sum_kernel,
        out_shape=jax.ShapeDtypeStruct((peers, PAGE, HEAD_DIM), half),
        in_specs=[SMEM, VMEM],
        out_specs=VMEM,
        compiler_params=small(8),
        name="sum",
    )(source, parts)
    returned = lax.all_to_all(summed, "tok", 0, 0, tiled=True)
    return pl.pallas_call(
        unpack_kernel,
        out_shape=jax.ShapeDtypeStruct((tok_rows, HEAD_DIM), half),
        in_specs=[SMEM, VMEM],
        out_specs=VMEM,
        compiler_params=small(8),
        name="unpack",
    )(dest, returned)


def solution(mesh):
    placed = (
        P("tok", "head"),
        P("tok", "head"),
        P("tok", "head"),
        P("tok", "head"),
        P(None, "head"),
        P(None, "head"),
        P(None, "head"),
        P("head", None),
        P(),
    )
    return jax.shard_map(
        per_device, mesh=mesh, in_specs=placed, out_specs=P("tok", "head"), check_vma=False
    )
```
